256 devices in a mesh: section: 8 (over x, core), row: 8 (over y, z_lo), col: 4 (over z_hi).
Axes of the slice: x: 4, y: 4, z: 8 (z_hi: 4, z_lo: 2; z = z_hi * 2 + z_lo), core: 2. Of those that a mesh axis runs over, the one named last changes fastest.
Arguments:
- tokens: bfloat16 [4096, 4096], P(('section', 'col'), 'row'), may hold values from -6 to 6
- grad_gate: bfloat16 [8, 8, 128, 14336], P('section', None, 'row', 'col'), may hold values from -0.5 to 0.5
- grad_up: bfloat16 [8, 8, 128, 14336], P('section', None, 'row', 'col'), may hold values from -0.5 to 0.5
- slot_token: int32 [8, 8, 128], P('section'), may hold values from 0 to 511, as said below
Outputs:
- gate_weight_grad: bfloat16 [8, 4096, 14336], P('section', 'row', 'col')
- up_weight_grad: bfloat16 [8, 4096, 14336], P('section', 'row', 'col')
The draws below stay inside these ranges and needn't reach their ends.
Inputs may be any that keep to these rules, and one draw needn't show every extreme that they name: slot_token[g, e, c] is a token of group g; every token of a group fills exactly two of its group's 8 * 128 slots, and every slot is filled.
All inputs are finite; a program needn't handle non-finite values.
Results may differ from the reference program's by a relative error of at most 0.001.
Values may be sent and summed in bfloat16 or wider, within the bound.
A program may use at most 256 MiB of HBM per device.

```python
import jax
import jax.numpy as jnp
from jax import lax

D = 4096
FF = 14336
E = 8
TOK_SECTION = 512
CAP = 128
TOKENS = 4096
N_SECTION = 8


def draw_slot_token(key, part):

    def draw_group(group_id):
        shuffled = jax.random.permutation(jax.random.fold_in(key, group_id), 2 * TOK_SECTION)
        return (shuffled % TOK_SECTION).reshape(E, CAP)
    return jax.vmap(draw_group)(jnp.arange(TOKENS // TOK_SECTION)).astype(jnp.int32)


def block_levels(own_key, extent, shards, low, top_value):
    gain, own = 1.0, jax.random.fold_in(own_key, 6)
    for dim, blocks in shards:
        draws = jnp.exp(jax.random.uniform(jax.random.fold_in(own, dim), (blocks,), jnp.float32, low / len(shards), top_value / len(shards)))
        gain = gain * jnp.repeat(draws, extent[dim] // blocks).reshape([-1 if axis == dim else 1 for axis in range(len(extent))])
    return gain


def normal_values(rng, extent, width, most, pieces=(), held_as=jnp.bfloat16):
    array = jax.random.normal(rng, extent, jnp.float32) * width
    if len(pieces) > 0:
        array = block_levels(rng, extent, pieces, -0.22, 0.18) * array
    return jnp.clip(array, min=-most, max=most).astype(held_as)


def setup_inputs(seed: int = 0) -> dict:
    streams_of = jax.random.split(jax.random.key(seed), 5)
    return {
        "tokens": normal_values(streams_of[0], (TOKENS, D), 1.0, 6.0, ((0, 32), (1, 8))),
        "grad_gate": normal_values(streams_of[1], (N_SECTION, E, CAP, FF), ((2 * TOK_SECTION) ** -0.5), 0.5, ((0, 8), (2, 8), (3, 4))),
        "grad_up": normal_values(streams_of[2], (N_SECTION, E, CAP, FF), ((2 * TOK_SECTION) ** -0.5), 0.5, ((0, 8), (2, 8), (3, 4))),
        "slot_token": draw_slot_token(jax.random.fold_in(streams_of[4], 71), 0),
    }


def reference(tokens, grad_gate, grad_up, slot_token):
    groups = tokens.shape[0] // TOK_SECTION
    grouped = tokens.reshape(groups, TOK_SECTION, D)

    def one_expert(expert):
        chosen = slot_token[:, expert, :]
        picked = jax.vmap(lambda block, where: block[where])(grouped, chosen).astype(jnp.float32)
        gate_part = grad_gate[:, expert].astype(jnp.float32)
        up_part = grad_up[:, expert].astype(jnp.float32)
        gate_grad = jnp.einsum("gcd,gcf->df", picked, gate_part, precision=lax.Precision.HIGHEST)
        up_grad = jnp.einsum("gcd,gcf->df", picked, up_part, precision=lax.Precision.HIGHEST)
        return gate_grad.astype(jnp.bfloat16), up_grad.astype(jnp.bfloat16)

    gate_out, up_out = lax.map(one_expert, jnp.arange(E, dtype=jnp.int32))
    return gate_out, up_out
```

```python
import functools

import jax
import jax.numpy as jnp
from jax import lax
from jax.experimental import pallas as pl
from jax.experimental.pallas import tpu as pltpu
from jax.sharding import PartitionSpec as P

NC = 14
LEAD = 3


def y_first(c):
    m = lax.rem(c, 5)
    return (m == 0) | (m == 2)


def kernel(
    n_sec, n_col,
    tok_ref, gate_ref, up_ref, slot_ref, out_gate, out_up,
    grads, toks, picked, lhs,
    tok_send, tok_recv, pick_send, pick_recv, sec_send, sec_recv, row_send, row_recv,
):
    s, r, k = lax.axis_index("section"), lax.axis_index("row"), lax.axis_index("col")
    y, z = r // 2, lax.rem(r, 2)

    def row_at(yy, zz):
        return lax.rem(yy + 8, 4) * 2 + zz

    y_up, y_down, z_other = row_at(y + 1, z), row_at(y - 1, z), row_at(y, 1 - z)
    rows = gate_ref.shape[2]
    wide = grads.shape[3]
    half = NC // 2
    n_tok = tok_ref.shape[0]
    cap = slot_ref.shape[2]

    def block(c, who):
        return grads.at[c, :, pl.ds(pl.multiple_of(who * rows, rows), rows), :]

    def piece(c, group):
        return grads.at[c, group, pl.ds(pl.multiple_of(r * rows, rows), rows), :]

    def row_copy(c, who, to):
        return pltpu.make_async_remote_copy(
            src_ref=block(c, who), dst_ref=block(c, who),
            send_sem=row_send.at[c], recv_sem=row_recv.at[c, who], device_id={"row": to},
        )

    def arrived(c, who):
        row_copy(c, who, y_up).wait_recv()

    barrier = pltpu.get_barrier_semaphore()

    def greet(axis, me, n):
        def one(j, carry):
            pl.semaphore_signal(barrier, inc=1, device_id={axis: lax.rem(me + j, n)})
            return carry
        lax.fori_loop(1, n, one, 0)

    greet("section", s, n_sec)
    greet("col", k, n_col)
    for to in (y_up, y_down, z_other):
        pl.semaphore_signal(barrier, inc=1, device_id={"row": to})
    pl.semaphore_wait(barrier, n_sec + n_col + 1)

    def sec_issue(c):
        def from_ref(ref, first):
            cols = pl.ds(pl.multiple_of((c - first) * wide, wide), wide)

            def one(j, carry):
                to = lax.rem(s + j, n_sec)
                pltpu.make_async_remote_copy(
                    src_ref=ref.at[0, to, :, cols], dst_ref=piece(c, s),
                    send_sem=sec_send.at[c], recv_sem=sec_recv.at[c], device_id={"section": to},
                ).start()
                return carry
            lax.fori_loop(1, n_sec, one, 0)
            pltpu.make_async_copy(ref.at[0, s, :, cols], piece(c, s), sec_recv.at[c]).start()

        @pl.when(c < half)
        def _():
            from_ref(gate_ref, 0)

        @pl.when(c >= half)
        def _():
            from_ref(up_ref, half)

    def sec_wait(c):
        pltpu.make_async_remote_copy(
            src_ref=block(c, r), dst_ref=block(c, r), send_sem=sec_send.at[c],
            recv_sem=sec_recv.at[c], device_id={"section": lax.rem(s + 1, n_sec)},
        ).wait_recv()

    for c in range(LEAD):
        sec_issue(c)

    def tok_at(which):
        return toks.at[pl.ds(pl.multiple_of(which * n_tok, n_tok), n_tok), :]

    def tok_one(j, carry):
        pltpu.make_async_remote_copy(
            src_ref=tok_ref, dst_ref=tok_at(k), send_sem=tok_send, recv_sem=tok_recv,
            device_id={"col": lax.rem(k + j, n_col)},
        ).start()
        return carry
    lax.fori_loop(1, n_col, tok_one, 0)
    pltpu.make_async_copy(tok_ref, tok_at(k), tok_recv).start()

    def lhs_at(group):
        return lhs.at[:, pl.ds(pl.multiple_of(group * cap, cap), cap)]

    def pick():
        pltpu.make_async_remote_copy(
            src_ref=toks, dst_ref=toks, send_sem=tok_send, recv_sem=tok_recv,
            device_id={"col": lax.rem(k + 1, n_col)},
        ).wait_recv()
        turned = toks[...].T

        def one(e, carry):
            ids = lax.broadcasted_iota(jnp.int32, (toks.shape[0], cap), 0)
            chosen = (ids == slot_ref[0, pl.ds(e, 1), :]).astype(jnp.bfloat16)
            picked[e] = jnp.dot(turned, chosen, preferred_element_type=jnp.float32).astype(jnp.bfloat16)
            return carry
        lax.fori_loop(0, n_sec, one, 0)

    def pick_issue():
        def one(j, carry):
            to = lax.rem(s + j, n_sec)
            pltpu.make_async_remote_copy(
                src_ref=picked.at[to], dst_ref=lhs_at(s), send_sem=pick_send, recv_sem=pick_recv,
                device_id={"section": to},
            ).start()
            return carry
        lax.fori_loop(1, n_sec, one, 0)
        lhs[:, pl.ds(pl.multiple_of(s * cap, cap), cap)] = picked[s]

    def pick_wait():
        most = lhs.at[:, pl.ds(0, (n_sec - 1) * cap)]
        pltpu.make_async_remote_copy(
            src_ref=most, dst_ref=most, send_sem=pick_send, recv_sem=pick_recv,
            device_id={"section": lax.rem(s + 1, n_sec)},
        ).wait_recv()

    def own(c):
        sec_wait(c)
        row_copy(c, r, z_other).start()
        row_copy(c, r, y_up).start()
        row_copy(c, r, y_down).start()

    def first(c):
        across = y_first(c)

        @pl.when(across)
        def _():
            arrived(c, y_down)
            row_copy(c, y_down, z_other).start()

            @pl.when(lax.rem(c, 5) == 0)
            def _():
                row_copy(c, y_down, y_up).start()
            arrived(c, y_up)
            row_copy(c, y_up, z_other).start()

            @pl.when(lax.rem(c, 5) != 0)
            def _():
                row_copy(c, y_up, y_down).start()

        @pl.when(jnp.logical_not(across))
        def _():
            arrived(c, z_other)
            row_copy(c, z_other, y_up).start()
            row_copy(c, z_other, y_down).start()
            arrived(c, y_down)
            row_copy(c, y_down, y_up).start()

    far, far_other = row_at(y + 2, z), row_at(y + 2, 1 - z)
    up_other, down_other = row_at(y + 1, 1 - z), row_at(y - 1, 1 - z)

    def second(c):
        across = y_first(c)

        @pl.when(across)
        def _():
            arrived(c, far)
            row_copy(c, far, z_other).start()

        @pl.when(jnp.logical_not(across))
        def _():
            arrived(c, up_other)
            row_copy(c, up_other, y_down).start()

    def finish(c):
        across = y_first(c)

        @pl.when(across)
        def _():
            arrived(c, z_other)
            arrived(c, up_other)

        @pl.when(jnp.logical_not(across))
        def _():
            arrived(c, y_up)
            arrived(c, far)
        arrived(c, down_other)
        arrived(c, far_other)
        summed = jnp.dot(
            lhs[...], grads[c].reshape(lhs.shape[1], wide), preferred_element_type=jnp.float32
        ).astype(jnp.bfloat16)

        @pl.when(c < half)
        def _():
            out_gate[0, :, pl.ds(pl.multiple_of(c * wide, wide), wide)] = summed

        @pl.when(c >= half)
        def _():
            out_up[0, :, pl.ds(pl.multiple_of((c - half) * wide, wide), wide)] = summed

    def step(t, carry):
        @pl.when(t + LEAD < NC)
        def _():
            sec_issue(t + LEAD)

        @pl.when(t < NC)
        def _():
            own(t)

        @pl.when((t >= 1) & (t < NC + 1))
        def _():
            first(t - 1)

        @pl.when((t >= 2) & (t < NC + 2))
        def _():
            second(t - 2)

        @pl.when(t == 1)
        def _():
            pick()

        @pl.when(t == 2)
        def _():
            pick_issue()

        @pl.when(t == 3)
        def _():
            pick_wait()

        @pl.when(t >= 3)
        def _():
            finish(t - 3)
        return carry
    lax.fori_loop(0, NC + 3, step, 0)

    def sent(ref, sem):
        pltpu.make_async_remote_copy(
            src_ref=ref, dst_ref=ref, send_sem=sem, recv_sem=row_recv.at[0, 0], device_id={"row": y_up},
        ).wait_send()

    sent(toks.at[pl.ds(0, (n_col - 1) * n_tok), :], tok_send)
    sent(lhs.at[:, pl.ds(0, (n_sec - 1) * cap)], pick_send)

    def drain(c, carry):
        sent(grads.at[c, pl.ds(0, n_sec - 1), pl.ds(0, rows), :], sec_send.at[c])
        sent(grads.at[c, :, pl.ds(0, 7 * rows), :], row_send.at[c])
        return carry
    lax.fori_loop(0, NC, drain, 0)


def body(n_sec, n_col, tokens, grad_gate, grad_up, slot_token):
    n_tok, d = tokens.shape
    _, e, rows, f = grad_gate.shape
    cap = slot_token.shape[2]
    wide = 2 * f // NC
    n_row = cap // rows
    dma = pltpu.SemaphoreType.DMA
    any_space = pl.BlockSpec(memory_space=pl.ANY)
    vmem = pl.BlockSpec(memory_space=pltpu.VMEM)
    return pl.pallas_call(
        functools.partial(kernel, n_sec, n_col),
        out_shape=(
            pltpu.VMEM((1, d, f), jnp.bfloat16),
            pltpu.VMEM((1, d, f), jnp.bfloat16),
        ),
        in_specs=[any_space, any_space, any_space, vmem],
        out_specs=(vmem, vmem),
        scratch_shapes=[
            pltpu.VMEM((NC, n_sec, cap, wide), jnp.bfloat16),
            pltpu.VMEM((n_tok * n_col, d), jnp.bfloat16),
            pltpu.VMEM((e, d, cap), jnp.bfloat16),
            pltpu.VMEM((d, n_sec * cap), jnp.bfloat16),
            dma(()), dma(()), dma(()), dma(()),
            dma((NC,)), dma((NC,)), dma((NC,)), dma((NC, n_row)),
        ],
        compiler_params=pltpu.CompilerParams(
            collective_id=0, has_side_effects=True, vmem_limit_bytes=50 * 2**20
        ),
        cost_estimate=pl.CostEstimate(
            flops=4 * n_sec * cap * d * f, bytes_accessed=4 * d * f, transcendentals=0
        ),
    )(tokens, grad_gate, grad_up, slot_token)


def solution(mesh):
    return jax.shard_map(
        functools.partial(body, mesh.shape["section"], mesh.shape["col"]),
        mesh=mesh,
        in_specs=(
            P(("section", "col"), "row"),
            P("section", None, "row", "col"),
            P("section", None, "row", "col"),
            P("section", None, None),
        ),
        out_specs=(P("section", "row", "col"), P("section", "row", "col")),
        check_vma=False,
    )
```

```python
import functools

import jax
import jax.numpy as jnp
from jax import lax
from jax.experimental import pallas as pl
from jax.experimental.pallas import tpu as pltpu
from jax.sharding import PartitionSpec as P

NC = 14
PAIRS = 4
LEAD = 4
LAG1, LAG2, LAG3 = 4, 5, 6
OTHER0, OWN0 = 8, 10


def pair_start(q):
    return 2 * q + jnp.maximum(q - 1, 0)


def paired(c):
    return (c < 4) | ((c >= 5) & (c < 10) & (lax.rem(c - 5, 3) != 2))


def plane(c):
    return jnp.where(c < 4, lax.rem(c, 2), lax.rem(c - 5, 3))


def kernel(
    n_sec, n_col,
    tok_ref, gate_ref, up_ref, slot_ref, out_gate, out_up,
    grads, toks, chosen, picked, lhs, stage,
    tok_send, tok_recv, pick_send, pick_recv, sec_send, sec_recv, row_send, row_recv, out_send, out_recv,
):
    s, r, k = lax.axis_index("section"), lax.axis_index("row"), lax.axis_index("col")
    y, z = r // 2, lax.rem(r, 2)

    def row_at(yy, zz):
        return lax.rem(yy + 8, 4) * 2 + zz

    y_up, y_down, z_other = row_at(y + 1, z), row_at(y - 1, z), row_at(y, 1 - z)
    far, far_other = row_at(y + 2, z), row_at(y + 2, 1 - z)
    up_other, down_other = row_at(y + 1, 1 - z), row_at(y - 1, 1 - z)
    rows = gate_ref.shape[2]
    wide = grads.shape[3]
    deep = out_gate.shape[1]
    half = NC // 2
    n_tok = tok_ref.shape[0]
    cap = slot_ref.shape[2]

    n_ring = 2 * n_col
    here = k * 2 + z

    def ring_device(w):
        w = lax.rem(w + n_ring, n_ring)
        return {"row": y * 2 + lax.rem(w, 2), "col": w // 2}

    def block(c, who):
        return grads.at[c, :, pl.ds(pl.multiple_of(who * rows, rows), rows), :]

    def piece(c, group):
        return grads.at[c, group, pl.ds(pl.multiple_of(r * rows, rows), rows), :]

    def row_copy(c, who, to):
        return pltpu.make_async_remote_copy(
            src_ref=block(c, who), dst_ref=block(c, who),
            send_sem=row_send.at[c], recv_sem=row_recv.at[c, who], device_id={"row": to},
        )

    def arrived(c, who):
        row_copy(c, who, y_up).wait_recv()

    barrier = pltpu.get_barrier_semaphore()

    def greet(j, carry):
        pl.semaphore_signal(barrier, inc=1, device_id={"section": lax.rem(s + j, n_sec)})
        return carry
    lax.fori_loop(1, n_sec, greet, 0)
    for to in (y_up, y_down):
        pl.semaphore_signal(barrier, inc=1, device_id={"row": to})
    for w in (here + 1, here - 1):
        pl.semaphore_signal(barrier, inc=1, device_id=ring_device(w))

    for e in range(n_sec):
        ids = lax.broadcasted_iota(jnp.int32, (toks.shape[1], cap), 0)
        chosen[:, e * cap : (e + 1) * cap] = (ids == slot_ref[0, e : e + 1, :]).astype(jnp.bfloat16)

    pl.semaphore_wait(barrier, n_sec + 3)

    def tok_at(w):
        w = lax.rem(w + n_ring, n_ring)
        return toks.at[lax.rem(w, 2), pl.ds(pl.multiple_of(w // 2 * n_tok, n_tok), n_tok), :]

    def tok_copy(w, way, src=None):
        return pltpu.make_async_remote_copy(
            src_ref=tok_at(w) if src is None else src, dst_ref=tok_at(w),
            send_sem=tok_send.at[way], recv_sem=tok_recv.at[lax.rem(w + n_ring, n_ring)],
            device_id=ring_device(here + 1 - 2 * way),
        )

    def tok_wait(w):
        tok_copy(w, 0).wait_recv()

    def tok_pass(h):
        tok_wait(here - h)

        @pl.when(h < n_ring // 2)
        def _():
            tok_copy(here - h, 0).start()

        @pl.when(h < n_ring // 2)
        def _():
            tok_wait(here + h)

        @pl.when(h < n_ring // 2 - 1)
        def _():
            tok_copy(here + h, 1).start()

    tok_copy(here, 0, tok_ref).start()
    tok_copy(here, 1, tok_ref).start()
    tok_own = pltpu.make_async_copy(tok_ref, tok_at(here), tok_recv.at[here])
    tok_own.start()

    def sec_issue(c):
        def from_ref(ref, first_chunk):
            cols = pl.ds(pl.multiple_of((c - first_chunk) * wide, wide), wide)

            def one(j, carry):
                to = lax.rem(s + j, n_sec)
                pltpu.make_async_remote_copy(
                    src_ref=ref.at[0, to, :, cols], dst_ref=piece(c, s),
                    send_sem=sec_send.at[c], recv_sem=sec_recv.at[c], device_id={"section": to},
                ).start()
                return carry
            lax.fori_loop(1, n_sec, one, 0)
            pltpu.make_async_copy(ref.at[0, s, :, cols], piece(c, s), sec_recv.at[c]).start()

        @pl.when(c < half)
        def _():
            from_ref(gate_ref, 0)

        @pl.when(c >= half)
        def _():
            from_ref(up_ref, half)

    def sec_wait(c):
        pltpu.make_async_remote_copy(
            src_ref=block(c, r), dst_ref=block(c, r), send_sem=sec_send.at[c],
            recv_sem=sec_recv.at[c], device_id={"section": lax.rem(s + 1, n_sec)},
        ).wait_recv()

    for c in range(LEAD):
        sec_issue(c)

    def features(which):
        return lax.rem(z + 1 + which, 2)

    def lhs_at(which, group):
        return lhs.at[which, :, pl.ds(pl.multiple_of(group * cap, cap), cap)]

    def pick(which):
        found = jnp.dot(
            toks[features(which)].T, chosen[...], preferred_element_type=jnp.float32
        ).astype(jnp.bfloat16)
        for e in range(n_sec):
            picked[which, e] = found[:, e * cap : (e + 1) * cap]

    def pick_issue(which):
        def one(j, carry):
            to = lax.rem(s + j, n_sec)
            pltpu.make_async_remote_copy(
                src_ref=picked.at[which, to], dst_ref=lhs_at(which, s), send_sem=pick_send.at[which],
                recv_sem=pick_recv.at[which], device_id={"section": to},
            ).start()
            return carry
        lax.fori_loop(1, n_sec, one, 0)
        lhs[which, :, pl.ds(pl.multiple_of(s * cap, cap), cap)] = picked[which, s]

    def pick_wait(which):
        most = lhs.at[which, :, pl.ds(0, (n_sec - 1) * cap)]
        pltpu.make_async_remote_copy(
            src_ref=most, dst_ref=most, send_sem=pick_send.at[which], recv_sem=pick_recv.at[which],
            device_id={"section": lax.rem(s + 1, n_sec)},
        ).wait_recv()

    def active(c):
        return jnp.logical_not(paired(c)) | (plane(c) == z)

    def own(c):
        sec_wait(c)

        @pl.when(jnp.logical_not(paired(c)) | (plane(c) != z))
        def _():
            row_copy(c, r, z_other).start()

        @pl.when(active(c))
        def _():
            row_copy(c, r, y_up).start()
            row_copy(c, r, y_down).start()

    def first(c):
        @pl.when(active(c))
        def _():
            arrived(c, z_other)
            row_copy(c, z_other, y_up).start()
            row_copy(c, z_other, y_down).start()
            arrived(c, y_down)
            row_copy(c, y_down, y_up).start()

    def second(c):
        @pl.when(active(c))
        def _():
            arrived(c, up_other)
            row_copy(c, up_other, y_down).start()

    def rest(c):
        for who in (y_up, far, down_other, far_other):
            arrived(c, who)

    def product(which, c):
        return jnp.dot(
            lhs[which], grads[c].reshape(lhs.shape[2], wide), preferred_element_type=jnp.float32
        ).astype(jnp.bfloat16)

    def columns(c, do):
        @pl.when(c < half)
        def _():
            do(out_gate, pl.ds(pl.multiple_of(c * wide, wide), wide))

        @pl.when(c >= half)
        def _():
            do(out_up, pl.ds(pl.multiple_of((c - half) * wide, wide), wide))

    def product_own(c):
        summed = product(1, c)

        def put(ref, cols):
            ref[0, :, cols] = summed
        columns(c, put)

    def out_issue(q, part):
        part_rows = pl.ds(part * (deep // 2), deep // 2)

        def send(ref, cols):
            pltpu.make_async_remote_copy(
                src_ref=stage.at[q, part_rows, :], dst_ref=ref.at[0, part_rows, cols],
                send_sem=out_send.at[q], recv_sem=out_recv.at[q], device_id={"row": z_other},
            ).start()
        columns(pair_start(q) + z, send)

    def out_copy(q):
        return pltpu.make_async_remote_copy(
            src_ref=stage.at[q], dst_ref=stage.at[q], send_sem=out_send.at[q], recv_sem=out_recv.at[q],
            device_id={"row": z_other},
        )

    def other_step(q):
        return jnp.maximum(pair_start(q) + LAG2 + 1, OTHER0)

    def own_step(q):
        return jnp.maximum(pair_start(q) + LAG2 + 3, OWN0 + q)

    def step(t, carry):
        @pl.when(t + LEAD < NC)
        def _():
            sec_issue(t + LEAD)

        @pl.when(t < NC)
        def _():
            own(t)

        @pl.when(t == 0)
        def _():
            tok_pass(1)

        @pl.when(t == 3)
        def _():
            tok_pass(2)

        @pl.when(t == 5)
        def _():
            if n_ring // 2 > 2:
                tok_pass(3)
            pick(0)
            pick_issue(0)

        @pl.when(t == 6)
        def _():
            if n_ring // 2 > 3:
                tok_pass(4)
            tok_own.wait()
            pick(1)

        @pl.when(t == 7)
        def _():
            pick_issue(1)

        @pl.when((t >= LAG1) & (t < NC + LAG1))
        def _():
            first(t - LAG1)

        @pl.when((t >= LAG2) & (t < NC + LAG2))
        def _():
            second(t - LAG2)

        def pair(q, carry):
            for part in range(2):
                @pl.when(t == other_step(q) + 1 + part)
                def _():
                    out_issue(q, part)

            @pl.when(t == other_step(q))
            def _():
                @pl.when(q == 0)
                def _():
                    pick_wait(0)
                rest(pair_start(q) + z)
                stage[q] = product(0, pair_start(q) + z)

            @pl.when(t == own_step(q))
            def _():
                product_own(pair_start(q) + z)
            return carry

        @pl.when(t == OWN0)
        def _():
            pick_wait(1)
        lax.fori_loop(0, PAIRS, pair, 0)

        plain = t - LAG3

        @pl.when((t >= OWN0) & jnp.logical_not(paired(plain)))
        def _():
            rest(plain)
            product_own(plain)
        return carry
    lax.fori_loop(0, NC + LAG3, step, 0)

    def sent(ref, sem):
        pltpu.make_async_remote_copy(
            src_ref=ref, dst_ref=ref, send_sem=sem, recv_sem=row_recv.at[0, 0], device_id={"row": y_up},
        ).wait_send()

    def drain_out(q, carry):
        out_copy(q).wait_recv()
        out_copy(q).wait_send()
        return carry
    lax.fori_loop(0, PAIRS, drain_out, 0)

    sent(toks.at[0], tok_send.at[0])
    sent(toks.at[0, pl.ds(0, (n_col - 1) * n_tok), :], tok_send.at[1])
    for which in range(2):
        sent(lhs.at[which, :, pl.ds(0, (n_sec - 1) * cap)], pick_send.at[which])

    def drain(c, carry):
        sent(grads.at[c, pl.ds(0, n_sec - 1), pl.ds(0, rows), :], sec_send.at[c])

        @pl.when(jnp.logical_not(paired(c)))
        def _():
            sent(grads.at[c, :, pl.ds(0, 7 * rows), :], row_send.at[c])

        @pl.when(paired(c) & active(c))
        def _():
            sent(grads.at[c, :, pl.ds(0, 6 * rows), :], row_send.at[c])

        @pl.when(jnp.logical_not(active(c)))
        def _():
            sent(grads.at[c, :, pl.ds(0, rows), :], row_send.at[c])
        return carry
    lax.fori_loop(0, NC, drain, 0)


def body(n_sec, n_col, tokens, grad_gate, grad_up, slot_token):
    n_tok, d = tokens.shape
    _, e, rows, f = grad_gate.shape
    cap = slot_token.shape[2]
    wide = 2 * f // NC
    n_row = cap // rows
    dma = pltpu.SemaphoreType.DMA
    any_space = pl.BlockSpec(memory_space=pl.ANY)
    vmem = pl.BlockSpec(memory_space=pltpu.VMEM)
    return pl.pallas_call(
        functools.partial(kernel, n_sec, n_col),
        out_shape=(
            pltpu.VMEM((1, d, f), jnp.bfloat16),
            pltpu.VMEM((1, d, f), jnp.bfloat16),
        ),
        in_specs=[any_space, any_space, any_space, vmem],
        out_specs=(vmem, vmem),
        scratch_shapes=[
            pltpu.VMEM((NC, n_sec, cap, wide), jnp.bfloat16),
            pltpu.VMEM((2, n_tok * n_col, d), jnp.bfloat16),
            pltpu.VMEM((n_tok * n_col, n_sec * cap), jnp.bfloat16),
            pltpu.VMEM((2, e, d, cap), jnp.bfloat16),
            pltpu.VMEM((2, d, n_sec * cap), jnp.bfloat16),
            pltpu.VMEM((PAIRS, d, wide), jnp.bfloat16),
            dma((2,)), dma((2 * n_col,)), dma((2,)), dma((2,)),
            dma((NC,)), dma((NC,)), dma((NC,)), dma((NC, n_row)), dma((PAIRS,)), dma((PAIRS,)),
        ],
        compiler_params=pltpu.CompilerParams(
            collective_id=0, has_side_effects=True, vmem_limit_bytes=50 * 2**20
        ),
        cost_estimate=pl.CostEstimate(
            flops=4 * n_sec * cap * d * f, bytes_accessed=4 * d * f, transcendentals=0
        ),
    )(tokens, grad_gate, grad_up, slot_token)


def solution(mesh):
    return jax.shard_map(
        functools.partial(body, mesh.shape["section"], mesh.shape["col"]),
        mesh=mesh,
        in_specs=(
            P(("section", "col"), "row"),
            P("section", None, "row", "col"),
            P("section", None, "row", "col"),
            P("section", None, None),
        ),
        out_specs=(P("section", "row", "col"), P("section", "row", "col")),
        check_vma=False,
    )
```

```python
import functools

import jax
import jax.numpy as jnp
from jax import lax
from jax.experimental import pallas as pl
from jax.experimental.pallas import tpu as pltpu
from jax.sharding import PartitionSpec as P

NC = 14
LOOP = NC - 1
PAIRS = 4
BEGIN = 6
AHEAD = 3
LEAD = 6
BEHIND = 11
LAGZ, LAG1, LAG2, LAG3 = 2, 4, 5, 6
OTHER0, OWN0 = 7, 10


def pair_start(q):
    return 2 * q


def paired(c):
    return c < 2 * PAIRS


def plane(c):
    return lax.rem(lax.rem(c, 2) + c // 2, 2)


def kernel(
    n_sec, n_col,
    tok_ref, gate_ref, up_ref, slot_ref, out_gate, out_up,
    grads, toks, chosen, picked, lhs, stage,
    tok_send, tok_recv, pick_send, pick_recv, sec_send, sec_recv, row_send, row_recv, out_send, out_recv,
):
    s, r, k = lax.axis_index("section"), lax.axis_index("row"), lax.axis_index("col")
    y, z = r // 2, lax.rem(r, 2)

    def row_at(yy, zz):
        return lax.rem(yy + 8, 4) * 2 + zz

    y_up, y_down, z_other = row_at(y + 1, z), row_at(y - 1, z), row_at(y, 1 - z)
    far, far_other = row_at(y + 2, z), row_at(y + 2, 1 - z)
    up_other, down_other = row_at(y + 1, 1 - z), row_at(y - 1, 1 - z)
    rows = gate_ref.shape[2]
    wide = grads.shape[3]
    deep = out_gate.shape[1]
    half = NC // 2
    n_tok = tok_ref.shape[0]
    cap = slot_ref.shape[2]

    n_ring = 2 * n_col
    here = k * 2 + z

    def ring_device(w):
        w = lax.rem(w + n_ring, n_ring)
        return {"row": y * 2 + lax.rem(w, 2), "col": w // 2}

    def block(c, who):
        return grads.at[c, :, pl.ds(pl.multiple_of(who * rows, rows), rows), :]

    def piece(c, group):
        return grads.at[c, group, pl.ds(pl.multiple_of(r * rows, rows), rows), :]

    def row_copy(c, who, to):
        return pltpu.make_async_remote_copy(
            src_ref=block(c, who), dst_ref=block(c, who),
            send_sem=row_send.at[c], recv_sem=row_recv.at[c, who], device_id={"row": to},
        )

    def arrived(c, who):
        row_copy(c, who, y_up).wait_recv()

    barrier = pltpu.get_barrier_semaphore()

    def greet(j, carry):
        pl.semaphore_signal(barrier, inc=1, device_id={"section": lax.rem(s + j, n_sec)})
        return carry
    lax.fori_loop(1, n_sec, greet, 0)
    for to in (y_up, y_down):
        pl.semaphore_signal(barrier, inc=1, device_id={"row": to})
    for w in (here + 1, here - 1):
        pl.semaphore_signal(barrier, inc=1, device_id=ring_device(w))

    for e in range(n_sec):
        ids = lax.broadcasted_iota(jnp.int32, (toks.shape[1], cap), 0)
        chosen[:, e * cap : (e + 1) * cap] = (ids == slot_ref[0, e : e + 1, :]).astype(jnp.bfloat16)

    pl.semaphore_wait(barrier, n_sec + 3)

    def tok_at(w):
        w = lax.rem(w + n_ring, n_ring)
        return toks.at[lax.rem(w, 2), pl.ds(pl.multiple_of(w // 2 * n_tok, n_tok), n_tok), :]

    def tok_copy(w, way, src=None):
        return pltpu.make_async_remote_copy(
            src_ref=tok_at(w) if src is None else src, dst_ref=tok_at(w),
            send_sem=tok_send.at[way], recv_sem=tok_recv.at[lax.rem(w + n_ring, n_ring)],
            device_id=ring_device(here + 1 - 2 * way),
        )

    def tok_wait(w):
        tok_copy(w, 0).wait_recv()

    def tok_pass(h):
        tok_wait(here - h)

        @pl.when(h < n_ring // 2)
        def _():
            tok_copy(here - h, 0).start()

        @pl.when(h < n_ring // 2)
        def _():
            tok_wait(here + h)

        @pl.when(h < n_ring // 2 - 1)
        def _():
            tok_copy(here + h, 1).start()

    tok_copy(here, 0, tok_ref).start()
    tok_copy(here, 1, tok_ref).start()
    tok_own = pltpu.make_async_copy(tok_ref, tok_at(here), tok_recv.at[here])
    tok_own.start()

    def sec_issue(c):
        def from_ref(ref, first_chunk):
            cols = pl.ds(pl.multiple_of((c - first_chunk) * wide, wide), wide)

            def one(j, carry):
                to = lax.rem(s + j, n_sec)
                pltpu.make_async_remote_copy(
                    src_ref=ref.at[0, to, :, cols], dst_ref=piece(c, s),
                    send_sem=sec_send.at[c], recv_sem=sec_recv.at[c], device_id={"section": to},
                ).start()
                return carry
            lax.fori_loop(1, n_sec, one, 0)
            pltpu.make_async_copy(ref.at[0, s, :, cols], piece(c, s), sec_recv.at[c]).start()

        @pl.when(c < half)
        def _():
            from_ref(gate_ref, 0)

        @pl.when(c >= half)
        def _():
            from_ref(up_ref, half)

    def sec_wait(c):
        pltpu.make_async_remote_copy(
            src_ref=block(c, r), dst_ref=block(c, r), send_sem=sec_send.at[c],
            recv_sem=sec_recv.at[c], device_id={"section": lax.rem(s + 1, n_sec)},
        ).wait_recv()

    open_cols = pl.ds((half - 1) * wide, wide)
    open_own = pltpu.make_async_copy(up_ref.at[0, :, :, open_cols], block(NC, r), row_recv.at[NC, r])
    open_own.start()
    for to in (y_up, y_down, z_other):
        pltpu.make_async_remote_copy(
            src_ref=up_ref.at[0, :, :, open_cols], dst_ref=block(NC, r),
            send_sem=row_send.at[NC], recv_sem=row_recv.at[NC, r], device_id={"row": to},
        ).start()

    for c in range(LEAD):
        sec_issue(c)

    def features(which):
        return lax.rem(z + 1 + which, 2)

    def lhs_at(which, group):
        return lhs.at[which, :, pl.ds(pl.multiple_of(group * cap, cap), cap)]

    def pick(which):
        found = jnp.dot(
            toks[features(which)].T, chosen[...], preferred_element_type=jnp.float32
        ).astype(jnp.bfloat16)
        for e in range(n_sec):
            picked[which, e] = found[:, e * cap : (e + 1) * cap]

    def pick_issue(which):
        def one(j, carry):
            to = lax.rem(s + j, n_sec)
            pltpu.make_async_remote_copy(
                src_ref=picked.at[which, to], dst_ref=lhs_at(which, s), send_sem=pick_send.at[which],
                recv_sem=pick_recv.at[which], device_id={"section": to},
            ).start()
            return carry
        lax.fori_loop(1, n_sec, one, 0)
        lhs[which, :, pl.ds(pl.multiple_of(s * cap, cap), cap)] = picked[which, s]

    def pick_wait(which):
        most = lhs.at[which, :, pl.ds(0, (n_sec - 1) * cap)]
        pltpu.make_async_remote_copy(
            src_ref=most, dst_ref=most, send_sem=pick_send.at[which], recv_sem=pick_recv.at[which],
            device_id={"section": lax.rem(s + 1, n_sec)},
        ).wait_recv()

    def active(c):
        return jnp.logical_not(paired(c)) | (plane(c) == z)

    def own_z(c):
        @pl.when(jnp.logical_not(paired(c)) | (plane(c) != z))
        def _():
            row_copy(c, r, z_other).start()

    def own_y(c):
        @pl.when(active(c))
        def _():
            row_copy(c, r, y_up).start()
            row_copy(c, r, y_down).start()

    def other_y(c):
        arrived(c, z_other)
        row_copy(c, z_other, y_up).start()
        row_copy(c, z_other, y_down).start()

    def pass_up(c):
        arrived(c, y_down)
        row_copy(c, y_down, y_up).start()

    def pass_down(c):
        arrived(c, up_other)
        row_copy(c, up_other, y_down).start()

    def if_active(c, do):
        @pl.when(active(c))
        def _():
            do(c)

    def pass_both(c):
        pass_up(c)
        pass_down(c)

    def rest(c):
        for who in (y_up, far, down_other, far_other):
            arrived(c, who)

    def open_copy(to):
        return pltpu.make_async_remote_copy(
            src_ref=grads.at[NC, to], dst_ref=grads.at[LOOP, s],
            send_sem=sec_send.at[LOOP], recv_sem=sec_recv.at[LOOP], device_id={"section": to},
        )

    def open_exchange():
        open_own.wait()
        rest(NC)

        def one(j, carry):
            open_copy(lax.rem(s + j, n_sec)).start()
            return carry
        lax.fori_loop(1, n_sec, one, 0)
        grads[LOOP, s] = grads[NC, s]

    def open_most():
        most = grads.at[LOOP, pl.ds(0, n_sec - 1)]
        return pltpu.make_async_remote_copy(
            src_ref=most, dst_ref=most, send_sem=sec_send.at[LOOP], recv_sem=sec_recv.at[LOOP],
            device_id={"section": lax.rem(s + 1, n_sec)},
        )

    def open_finish():
        open_most().wait_recv()
        product_own(LOOP)

    def product(which, c):
        return jnp.dot(
            lhs[which], grads[c].reshape(lhs.shape[2], wide), preferred_element_type=jnp.float32
        ).astype(jnp.bfloat16)

    def columns(c, do):
        @pl.when(c < half)
        def _():
            do(out_gate, pl.ds(pl.multiple_of(c * wide, wide), wide))

        @pl.when(c >= half)
        def _():
            do(out_up, pl.ds(pl.multiple_of((c - half) * wide, wide), wide))

    def product_own(c):
        summed = product(1, c)

        def put(ref, cols):
            ref[0, :, cols] = summed
        columns(c, put)

    def out_issue(q):
        def send(ref, cols):
            pltpu.make_async_remote_copy(
                src_ref=stage.at[q], dst_ref=ref.at[0, :, cols],
                send_sem=out_send.at[q], recv_sem=out_recv.at[q], device_id={"row": z_other},
            ).start()
        columns(pair_start(q) + lax.rem(z + q, 2), send)

    def out_copy(q):
        return pltpu.make_async_remote_copy(
            src_ref=stage.at[q], dst_ref=stage.at[q], send_sem=out_send.at[q], recv_sem=out_recv.at[q],
            device_id={"row": z_other},
        )

    def other_step(q):
        return jnp.maximum(pair_start(q) + LAG2 + 1, OTHER0)

    def own_step(q):
        return jnp.maximum(pair_start(q) + LAG2 + 3, OWN0 + q)

    def step(t, carry):
        @pl.when(t + AHEAD < LOOP)
        def _():
            sec_wait(t + AHEAD)
            own_z(t + AHEAD)

        def out_step(q, carry):
            @pl.when(t == other_step(q) + 1)
            def _():
                out_issue(q)
            return carry
        lax.fori_loop(0, PAIRS, out_step, 0)

        @pl.when(t < LOOP)
        def _():
            own_y(t)

        @pl.when(t == BEGIN)
        def _():
            pick_issue(1)

        @pl.when(t < LOOP + LAGZ)
        def _():
            if_active(t - LAGZ, other_y)

        @pl.when(t < LOOP + LAG1)
        def _():
            if_active(t - LAG1, pass_both)

        @pl.when(t == BEGIN + 1)
        def _():
            open_exchange()

        @pl.when(t == LOOP)
        def _():
            open_finish()

        def pair(q, carry):
            @pl.when(t == other_step(q))
            def _():
                @pl.when(q == 0)
                def _():
                    pick_wait(0)
                rest(pair_start(q) + lax.rem(z + q, 2))
                stage[q] = product(0, pair_start(q) + lax.rem(z + q, 2))

            @pl.when(t == own_step(q))
            def _():
                product_own(pair_start(q) + lax.rem(z + q, 2))
            return carry

        @pl.when(t == OWN0)
        def _():
            pick_wait(1)
        lax.fori_loop(0, PAIRS, pair, 0)

        plain = t - LAG3

        @pl.when((t >= OWN0) & jnp.logical_not(paired(plain)))
        def _():
            rest(plain)
            product_own(plain)
        return carry

    tok_pass(1)
    sec_wait(0)
    own_z(0)
    own_y(0)
    pass_up(NC)
    sec_wait(1)
    own_z(1)
    own_y(1)
    other_y(NC)
    sec_issue(LEAD)
    sec_issue(LEAD + 1)
    sec_wait(2)
    own_y(2)
    tok_pass(2)
    for c in (3, 4):
        sec_wait(c)
        own_y(c)
    for c in range(LEAD + 2, BEHIND):
        sec_issue(c)
    if_active(0, other_y)
    if_active(1, other_y)
    pass_down(NC)
    if n_ring // 2 > 2:
        tok_pass(3)
    pick(0)
    for c in (2, 3, 4):
        own_z(c)
    pick_issue(0)
    for c in range(BEHIND, LOOP):
        sec_issue(c)
    for c in range(5, BEGIN + AHEAD):
        sec_wait(c)
        own_z(c)
        if c < BEGIN:
            own_y(c)
    if_active(0, pass_both)
    if_active(1, pass_both)
    if n_ring // 2 > 3:
        tok_pass(4)
    tok_own.wait()
    pick(1)
    if_active(2, other_y)
    if_active(3, other_y)
    lax.fori_loop(BEGIN, LOOP + LAG3, step, 0)

    def sent(ref, sem):
        pltpu.make_async_remote_copy(
            src_ref=ref, dst_ref=ref, send_sem=sem, recv_sem=row_recv.at[0, 0], device_id={"row": y_up},
        ).wait_send()

    def drain_out(q, carry):
        out_copy(q).wait_recv()
        out_copy(q).wait_send()
        return carry
    lax.fori_loop(0, PAIRS, drain_out, 0)

    sent(toks.at[0], tok_send.at[0])
    sent(toks.at[0, pl.ds(0, (n_col - 1) * n_tok), :], tok_send.at[1])
    for which in range(2):
        sent(lhs.at[which, :, pl.ds(0, (n_sec - 1) * cap)], pick_send.at[which])

    def drain(c, carry):
        sent(grads.at[c, pl.ds(0, n_sec - 1), pl.ds(0, rows), :], sec_send.at[c])

        @pl.when(jnp.logical_not(paired(c)))
        def _():
            sent(grads.at[c, :, pl.ds(0, 7 * rows), :], row_send.at[c])

        @pl.when(paired(c) & active(c))
        def _():
            sent(grads.at[c, :, pl.ds(0, 6 * rows), :], row_send.at[c])

        @pl.when(jnp.logical_not(active(c)))
        def _():
            sent(grads.at[c, :, pl.ds(0, rows), :], row_send.at[c])
        return carry
    lax.fori_loop(0, LOOP, drain, 0)
    open_most().wait_send()
    sent(grads.at[NC, :, pl.ds(0, 7 * rows), :], row_send.at[NC])


def body(n_sec, n_col, tokens, grad_gate, grad_up, slot_token):
    n_tok, d = tokens.shape
    _, e, rows, f = grad_gate.shape
    cap = slot_token.shape[2]
    wide = 2 * f // NC
    n_row = cap // rows
    dma = pltpu.SemaphoreType.DMA
    any_space = pl.BlockSpec(memory_space=pl.ANY)
    vmem = pl.BlockSpec(memory_space=pltpu.VMEM)
    return pl.pallas_call(
        functools.partial(kernel, n_sec, n_col),
        out_shape=(
            pltpu.VMEM((1, d, f), jnp.bfloat16),
            pltpu.VMEM((1, d, f), jnp.bfloat16),
        ),
        in_specs=[any_space, any_space, any_space, vmem],
        out_specs=(vmem, vmem),
        scratch_shapes=[
            pltpu.VMEM((NC + 1, n_sec, cap, wide), jnp.bfloat16),
            pltpu.VMEM((2, n_tok * n_col, d), jnp.bfloat16),
            pltpu.VMEM((n_tok * n_col, n_sec * cap), jnp.bfloat16),
            pltpu.VMEM((2, e, d, cap), jnp.bfloat16),
            pltpu.VMEM((2, d, n_sec * cap), jnp.bfloat16),
            pltpu.VMEM((PAIRS, d, wide), jnp.bfloat16),
            dma((2,)), dma((2 * n_col,)), dma((2,)), dma((2,)),
            dma((NC,)), dma((NC,)), dma((NC + 1,)), dma((NC + 1, n_row)), dma((PAIRS,)), dma((PAIRS,)),
        ],
        compiler_params=pltpu.CompilerParams(
            collective_id=0, has_side_effects=True, vmem_limit_bytes=50 * 2**20
        ),
        cost_estimate=pl.CostEstimate(
            flops=4 * n_sec * cap * d * f, bytes_accessed=4 * d * f, transcendentals=0
        ),
    )(tokens, grad_gate, grad_up, slot_token)


def solution(mesh):
    return jax.shard_map(
        functools.partial(body, mesh.shape["section"], mesh.shape["col"]),
        mesh=mesh,
        in_specs=(
            P(("section", "col"), "row"),
            P("section", None, "row", "col"),
            P("section", None, "row", "col"),
            P("section", None, None),
        ),
        out_specs=(P("section", "row", "col"), P("section", "row", "col")),
        check_vma=False,
    )
```

```python
import functools

import jax
import jax.numpy as jnp
from jax import lax
from jax.experimental import pallas as pl
from jax.experimental.pallas import tpu as pltpu
from jax.sharding import PartitionSpec as P

NC = 14
OPEN = 2
LOOP = NC - OPEN
PAIRS = 4
BEGIN = 6
AHEAD = 3
LEAD = 6
BEHIND = 11
LAGZ, LAG1, LAG2, LAG3 = 2, 4, 5, 6
OTHER0, OWN0 = 7, 10


def pair_start(q):
    return 2 * q


def paired(c):
    return c < 2 * PAIRS


def plane(c):
    return lax.rem(lax.rem(c, 2) + c // 2, 2)


def kernel(
    n_sec, n_col,
    tok_ref, gate_ref, up_ref, slot_ref, out_gate, out_up,
    grads, toks, chosen, picked, lhs, stage,
    tok_send, tok_recv, pick_send, pick_recv, sec_send, sec_recv, row_send, row_recv, out_send, out_recv,
):
    s, r, k = lax.axis_index("section"), lax.axis_index("row"), lax.axis_index("col")
    y, z = r // 2, lax.rem(r, 2)

    def row_at(yy, zz):
        return lax.rem(yy + 8, 4) * 2 + zz

    y_up, y_down, z_other = row_at(y + 1, z), row_at(y - 1, z), row_at(y, 1 - z)
    far, far_other = row_at(y + 2, z), row_at(y + 2, 1 - z)
    up_other, down_other = row_at(y + 1, 1 - z), row_at(y - 1, 1 - z)
    rows = gate_ref.shape[2]
    wide = grads.shape[3]
    deep = out_gate.shape[1]
    half = NC // 2
    n_tok = tok_ref.shape[0]
    cap = slot_ref.shape[2]

    n_ring = 2 * n_col
    here = k * 2 + z

    def ring_device(w):
        w = lax.rem(w + n_ring, n_ring)
        return {"row": y * 2 + lax.rem(w, 2), "col": w // 2}

    def block(c, who):
        return grads.at[c, :, pl.ds(pl.multiple_of(who * rows, rows), rows), :]

    def piece(c, group):
        return grads.at[c, group, pl.ds(pl.multiple_of(r * rows, rows), rows), :]

    def row_copy(c, who, to):
        return pltpu.make_async_remote_copy(
            src_ref=block(c, who), dst_ref=block(c, who),
            send_sem=row_send.at[c], recv_sem=row_recv.at[c, who], device_id={"row": to},
        )

    def arrived(c, who):
        row_copy(c, who, y_up).wait_recv()

    barrier = pltpu.get_barrier_semaphore()

    def greet(j, carry):
        pl.semaphore_signal(barrier, inc=1, device_id={"section": lax.rem(s + j, n_sec)})
        return carry
    lax.fori_loop(1, n_sec, greet, 0)
    for to in (y_up, y_down):
        pl.semaphore_signal(barrier, inc=1, device_id={"row": to})
    for w in (here + 1, here - 1):
        pl.semaphore_signal(barrier, inc=1, device_id=ring_device(w))

    for e in range(n_sec):
        ids = lax.broadcasted_iota(jnp.int32, (toks.shape[1], cap), 0)
        chosen[:, e * cap : (e + 1) * cap] = (ids == slot_ref[0, e : e + 1, :]).astype(jnp.bfloat16)

    pl.semaphore_wait(barrier, n_sec + 3)

    def tok_at(w):
        w = lax.rem(w + n_ring, n_ring)
        return toks.at[lax.rem(w, 2), pl.ds(pl.multiple_of(w // 2 * n_tok, n_tok), n_tok), :]

    def tok_copy(w, way, src=None):
        return pltpu.make_async_remote_copy(
            src_ref=tok_at(w) if src is None else src, dst_ref=tok_at(w),
            send_sem=tok_send.at[way], recv_sem=tok_recv.at[lax.rem(w + n_ring, n_ring)],
            device_id=ring_device(here + 1 - 2 * way),
        )

    def tok_wait(w):
        tok_copy(w, 0).wait_recv()

    def tok_pass(h):
        origin = lax.rem(here + h, 2)

        @pl.when(h <= n_col - origin)
        def _():
            tok_wait(here - h)

        @pl.when(h < n_col - origin)
        def _():
            tok_copy(here - h, 0).start()

        @pl.when(h <= n_col - 1 + origin)
        def _():
            tok_wait(here + h)

        @pl.when(h < n_col - 1 + origin)
        def _():
            tok_copy(here + h, 1).start()

    tok_copy(here, 0, tok_ref).start()
    tok_copy(here, 1, tok_ref).start()
    tok_own = pltpu.make_async_copy(tok_ref, tok_at(here), tok_recv.at[here])
    tok_own.start()

    def sec_issue(c):
        def from_ref(ref, first_chunk):
            cols = pl.ds(pl.multiple_of((c - first_chunk) * wide, wide), wide)

            def one(j, carry):
                to = lax.rem(s + j, n_sec)
                pltpu.make_async_remote_copy(
                    src_ref=ref.at[0, to, :, cols], dst_ref=piece(c, s),
                    send_sem=sec_send.at[c], recv_sem=sec_recv.at[c], device_id={"section": to},
                ).start()
                return carry
            lax.fori_loop(1, n_sec, one, 0)
            pltpu.make_async_copy(ref.at[0, s, :, cols], piece(c, s), sec_recv.at[c]).start()

        @pl.when(c < half)
        def _():
            from_ref(gate_ref, 0)

        @pl.when(c >= half)
        def _():
            from_ref(up_ref, half)

    def sec_wait(c):
        pltpu.make_async_remote_copy(
            src_ref=block(c, r), dst_ref=block(c, r), send_sem=sec_send.at[c],
            recv_sem=sec_recv.at[c], device_id={"section": lax.rem(s + 1, n_sec)},
        ).wait_recv()

    def open_src(i):
        return up_ref.at[0, :, :, pl.ds((half - OPEN + i) * wide, wide)]

    def open_local(i):
        return pltpu.make_async_copy(open_src(i), block(NC + i, r), row_recv.at[NC + i, r])

    def open_own(i, to):
        pltpu.make_async_remote_copy(
            src_ref=open_src(i), dst_ref=block(NC + i, r),
            send_sem=row_send.at[NC + i], recv_sem=row_recv.at[NC + i, r], device_id={"row": to},
        ).start()

    for i in range(OPEN):
        open_local(i).start()
        open_own(i, y_up)
        open_own(i, y_down)
    open_own(0, z_other)

    for c in range(LEAD):
        sec_issue(c)

    def features(which):
        return lax.rem(z + 1 + which, 2)

    def lhs_at(which, group):
        return lhs.at[which, :, pl.ds(pl.multiple_of(group * cap, cap), cap)]

    def pick(which):
        found = jnp.dot(
            toks[features(which)].T, chosen[...], preferred_element_type=jnp.float32
        ).astype(jnp.bfloat16)
        for e in range(n_sec):
            picked[which, e] = found[:, e * cap : (e + 1) * cap]

    def pick_issue(which):
        def one(j, carry):
            to = lax.rem(s + j, n_sec)
            pltpu.make_async_remote_copy(
                src_ref=picked.at[which, to], dst_ref=lhs_at(which, s), send_sem=pick_send.at[which],
                recv_sem=pick_recv.at[which], device_id={"section": to},
            ).start()
            return carry
        lax.fori_loop(1, n_sec, one, 0)
        lhs[which, :, pl.ds(pl.multiple_of(s * cap, cap), cap)] = picked[which, s]

    def pick_wait(which):
        most = lhs.at[which, :, pl.ds(0, (n_sec - 1) * cap)]
        pltpu.make_async_remote_copy(
            src_ref=most, dst_ref=most, send_sem=pick_send.at[which], recv_sem=pick_recv.at[which],
            device_id={"section": lax.rem(s + 1, n_sec)},
        ).wait_recv()

    def active(c):
        return jnp.logical_not(paired(c)) | (plane(c) == z)

    def own_z(c):
        @pl.when(jnp.logical_not(paired(c)) | (plane(c) != z))
        def _():
            row_copy(c, r, z_other).start()

    def own_y(c):
        @pl.when(active(c))
        def _():
            row_copy(c, r, y_up).start()
            row_copy(c, r, y_down).start()

    def other_y(c):
        arrived(c, z_other)
        row_copy(c, z_other, y_up).start()
        row_copy(c, z_other, y_down).start()

    def pass_up(c):
        arrived(c, y_down)
        row_copy(c, y_down, y_up).start()

    def pass_down(c):
        arrived(c, up_other)
        row_copy(c, up_other, y_down).start()

    def if_active(c, do):
        @pl.when(active(c))
        def _():
            do(c)

    def pass_both(c):
        pass_up(c)
        pass_down(c)

    def rest(c):
        for who in (y_up, far, down_other, far_other):
            arrived(c, who)

    def open_exchange(i):
        open_local(i).wait()
        rest(NC + i)

        def one(j, carry):
            to = lax.rem(s + j, n_sec)
            pltpu.make_async_remote_copy(
                src_ref=grads.at[NC + i, to], dst_ref=grads.at[LOOP + i, s],
                send_sem=sec_send.at[LOOP + i], recv_sem=sec_recv.at[LOOP + i], device_id={"section": to},
            ).start()
            return carry
        lax.fori_loop(1, n_sec, one, 0)
        grads[LOOP + i, s] = grads[NC + i, s]

    def open_most(i):
        most = grads.at[LOOP + i, pl.ds(0, n_sec - 1)]
        return pltpu.make_async_remote_copy(
            src_ref=most, dst_ref=most, send_sem=sec_send.at[LOOP + i], recv_sem=sec_recv.at[LOOP + i],
            device_id={"section": lax.rem(s + 1, n_sec)},
        )

    def open_finish(i):
        open_most(i).wait_recv()
        product_own(LOOP + i)

    def product(which, c):
        return jnp.dot(
            lhs[which], grads[c].reshape(lhs.shape[2], wide), preferred_element_type=jnp.float32
        ).astype(jnp.bfloat16)

    def columns(c, do):
        @pl.when(c < half)
        def _():
            do(out_gate, pl.ds(pl.multiple_of(c * wide, wide), wide))

        @pl.when(c >= half)
        def _():
            do(out_up, pl.ds(pl.multiple_of((c - half) * wide, wide), wide))

    def product_own(c):
        summed = product(1, c)

        def put(ref, cols):
            ref[0, :, cols] = summed
        columns(c, put)

    def out_issue(q):
        def send(ref, cols):
            pltpu.make_async_remote_copy(
                src_ref=stage.at[q], dst_ref=ref.at[0, :, cols],
                send_sem=out_send.at[q], recv_sem=out_recv.at[q], device_id={"row": z_other},
            ).start()
        columns(pair_start(q) + lax.rem(z + q, 2), send)

    def out_copy(q):
        return pltpu.make_async_remote_copy(
            src_ref=stage.at[q], dst_ref=stage.at[q], send_sem=out_send.at[q], recv_sem=out_recv.at[q],
            device_id={"row": z_other},
        )

    def other_step(q):
        return jnp.maximum(pair_start(q) + LAG2 + 1, OTHER0)

    def own_step(q):
        return jnp.maximum(pair_start(q) + LAG2 + 3, OWN0 + q)

    def step(t, carry):
        @pl.when(t + AHEAD < LOOP)
        def _():
            sec_wait(t + AHEAD)
            own_z(t + AHEAD)

        def out_step(q, carry):
            @pl.when(t == other_step(q) + 1)
            def _():
                out_issue(q)
            return carry
        lax.fori_loop(0, PAIRS, out_step, 0)

        @pl.when(t < LOOP)
        def _():
            own_y(t)

        @pl.when(t == BEGIN)
        def _():
            pick_issue(1)

        @pl.when(t < LOOP + LAGZ)
        def _():
            if_active(t - LAGZ, other_y)

        @pl.when(t < LOOP + LAG1)
        def _():
            if_active(t - LAG1, pass_both)

        for i in range(OPEN):
            @pl.when(t == BEGIN + 1 + i)
            def _():
                open_exchange(i)

        @pl.when((t >= LOOP) & (t < NC))
        def _():
            open_finish(t - LOOP)

        def pair(q, carry):
            @pl.when(t == other_step(q))
            def _():
                @pl.when(q == 0)
                def _():
                    pick_wait(0)
                rest(pair_start(q) + lax.rem(z + q, 2))
                stage[q] = product(0, pair_start(q) + lax.rem(z + q, 2))

            @pl.when(t == own_step(q))
            def _():
                product_own(pair_start(q) + lax.rem(z + q, 2))
            return carry

        @pl.when(t == OWN0)
        def _():
            pick_wait(1)
        lax.fori_loop(0, PAIRS, pair, 0)

        plain = t - LAG3

        @pl.when((t >= OWN0) & jnp.logical_not(paired(plain)))
        def _():
            rest(plain)
            product_own(plain)
        return carry

    tok_pass(1)
    for i in range(1, OPEN):
        open_own(i, z_other)
    sec_wait(0)
    own_z(0)
    own_y(0)
    pass_up(NC)
    sec_wait(1)
    own_z(1)
    own_y(1)
    other_y(NC)
    sec_issue(LEAD)
    sec_issue(LEAD + 1)
    sec_wait(2)
    own_y(2)
    for i in range(1, OPEN):
        pass_up(NC + i)
    tok_pass(2)
    for c in (3, 4):
        sec_wait(c)
        own_y(c)
    for c in range(LEAD + 2, BEHIND):
        sec_issue(c)
    for i in range(1, OPEN):
        other_y(NC + i)
    if_active(0, other_y)
    if_active(1, other_y)
    pass_down(NC)
    if n_ring // 2 > 2:
        tok_pass(3)
    pick(0)
    for c in (2, 3, 4):
        own_z(c)
    pick_issue(0)
    for c in range(BEHIND, LOOP):
        sec_issue(c)
    for c in range(5, BEGIN + AHEAD):
        sec_wait(c)
        own_z(c)
        if c < BEGIN:
            own_y(c)
    for i in range(1, OPEN):
        pass_down(NC + i)
    if_active(0, pass_both)
    if_active(1, pass_both)
    if n_ring // 2 > 3:
        tok_pass(4)
    tok_own.wait()
    pick(1)
    if_active(2, other_y)
    if_active(3, other_y)
    lax.fori_loop(BEGIN, LOOP + LAG3, step, 0)

    def sent(ref, sem):
        pltpu.make_async_remote_copy(
            src_ref=ref, dst_ref=ref, send_sem=sem, recv_sem=row_recv.at[0, 0], device_id={"row": y_up},
        ).wait_send()

    def drain_out(q, carry):
        out_copy(q).wait_recv()
        out_copy(q).wait_send()
        return carry
    lax.fori_loop(0, PAIRS, drain_out, 0)

    sent(toks.at[0, pl.ds(0, (n_col - 1) * n_tok), :], tok_send.at[z])
    sent(toks.at[0], tok_send.at[1 - z])
    for which in range(2):
        sent(lhs.at[which, :, pl.ds(0, (n_sec - 1) * cap)], pick_send.at[which])

    def drain(c, carry):
        sent(grads.at[c, pl.ds(0, n_sec - 1), pl.ds(0, rows), :], sec_send.at[c])

        @pl.when(jnp.logical_not(paired(c)))
        def _():
            sent(grads.at[c, :, pl.ds(0, 7 * rows), :], row_send.at[c])

        @pl.when(paired(c) & active(c))
        def _():
            sent(grads.at[c, :, pl.ds(0, 6 * rows), :], row_send.at[c])

        @pl.when(jnp.logical_not(active(c)))
        def _():
            sent(grads.at[c, :, pl.ds(0, rows), :], row_send.at[c])
        return carry
    lax.fori_loop(0, LOOP, drain, 0)
    for i in range(OPEN):
        open_most(i).wait_send()
        sent(grads.at[NC, :, pl.ds(0, 7 * rows), :], row_send.at[NC + i])


def body(n_sec, n_col, tokens, grad_gate, grad_up, slot_token):
    n_tok, d = tokens.shape
    _, e, rows, f = grad_gate.shape
    cap = slot_token.shape[2]
    wide = 2 * f // NC
    n_row = cap // rows
    dma = pltpu.SemaphoreType.DMA
    any_space = pl.BlockSpec(memory_space=pl.ANY)
    vmem = pl.BlockSpec(memory_space=pltpu.VMEM)
    gate, up = pl.pallas_call(
        functools.partial(kernel, n_sec, n_col),
        out_shape=(
            pltpu.VMEM((1, d, f), jnp.bfloat16),
            pltpu.VMEM((1, d, f), jnp.bfloat16),
        ),
        in_specs=[any_space, any_space, any_space, vmem],
        out_specs=(vmem, vmem),
        scratch_shapes=[
            pltpu.VMEM((NC + OPEN, n_sec, cap, wide), jnp.bfloat16),
            pltpu.VMEM((2, n_tok * n_col, d), jnp.bfloat16),
            pltpu.VMEM((n_tok * n_col, n_sec * cap), jnp.bfloat16),
            pltpu.VMEM((2, e, d, cap), jnp.bfloat16),
            pltpu.VMEM((2, d, n_sec * cap), jnp.bfloat16),
            pltpu.VMEM((PAIRS, d, wide), jnp.bfloat16),
            dma((2,)), dma((2 * n_col,)), dma((2,)), dma((2,)),
            dma((NC,)), dma((NC,)), dma((NC + OPEN,)), dma((NC + OPEN, n_row)), dma((PAIRS,)), dma((PAIRS,)),
        ],
        compiler_params=pltpu.CompilerParams(
            collective_id=0, has_side_effects=True, vmem_limit_bytes=50 * 2**20
        ),
        cost_estimate=pl.CostEstimate(
            flops=4 * n_sec * cap * d * f, bytes_accessed=4 * d * f, transcendentals=0
        ),
    )(tokens, grad_gate, grad_up, slot_token)
    shape = jax.ShapeDtypeStruct((1, d, f), jnp.bfloat16)
    return pl.pallas_call(
        settle,
        out_shape=(shape, shape),
        in_specs=[vmem, vmem],
        out_specs=(any_space, any_space),
        scratch_shapes=[dma((2,))],
        compiler_params=pltpu.CompilerParams(vmem_limit_bytes=2 * 2**20),
    )(gate, up)


def settle(gate_in, up_in, gate_out, up_out, sems):
    pieces = 8
    step = gate_in.shape[1] // pieces
    for j, (ref, out) in enumerate(((gate_in, gate_out), (up_in, up_out))):
        for i in range(pieces):
            rows = pl.ds(i * step, step)
            pltpu.make_async_copy(ref.at[:, rows, :], out.at[:, rows, :], sems.at[j]).start()
    pltpu.make_async_copy(gate_in, gate_out, sems.at[0]).wait()
    pltpu.make_async_copy(up_in, up_out, sems.at[1]).wait()


def solution(mesh):
    return jax.shard_map(
        functools.partial(body, mesh.shape["section"], mesh.shape["col"]),
        mesh=mesh,
        in_specs=(
            P(("section", "col"), "row"),
            P("section", None, "row", "col"),
            P("section", None, "row", "col"),
            P("section", None, None),
        ),
        out_specs=(P("section", "row", "col"), P("section", "row", "col")),
        check_vma=False,
    )
```

```python
import functools

import jax
import jax.numpy as jnp
from jax import lax
from jax.experimental import pallas as pl
from jax.experimental.pallas import tpu as pltpu
from jax.sharding import PartitionSpec as P

NC = 14
OPEN = 2
LOOP = NC - OPEN
PAIRS = 4
BEGIN = 6
AHEAD = 3
LEAD = 6
BEHIND = 11
LAGZ, LAG1, LAG2, LAG3 = 1, 4, 5, 6
OTHER0, OWN0 = 7, 10


def pair_start(q):
    return 2 * q


def paired(c):
    return c < 2 * PAIRS


def plane(c):
    return lax.rem(lax.rem(c, 2) + c // 2, 2)


def kernel(
    n_sec, n_col,
    tok_ref, gate_ref, up_ref, slot_ref, out_gate, out_up,
    grads, toks, chosen, picked, lhs, stage,
    tok_send, tok_recv, pick_send, pick_recv, sec_send, sec_recv, row_send, row_recv, out_send, out_recv,
):
    s, r, k = lax.axis_index("section"), lax.axis_index("row"), lax.axis_index("col")
    y, z = r // 2, lax.rem(r, 2)

    def row_at(yy, zz):
        return lax.rem(yy + 8, 4) * 2 + zz

    y_up, y_down, z_other = row_at(y + 1, z), row_at(y - 1, z), row_at(y, 1 - z)
    far, far_other = row_at(y + 2, z), row_at(y + 2, 1 - z)
    up_other, down_other = row_at(y + 1, 1 - z), row_at(y - 1, 1 - z)
    rows = gate_ref.shape[2]
    wide = grads.shape[3]
    deep = out_gate.shape[1]
    half = NC // 2
    n_tok = tok_ref.shape[0]
    cap = slot_ref.shape[2]

    n_ring = 2 * n_col
    here = k * 2 + z

    def ring_device(w):
        w = lax.rem(w + n_ring, n_ring)
        return {"row": y * 2 + lax.rem(w, 2), "col": w // 2}

    def block(c, who):
        return grads.at[c, :, pl.ds(pl.multiple_of(who * rows, rows), rows), :]

    def piece(c, group):
        return grads.at[c, group, pl.ds(pl.multiple_of(r * rows, rows), rows), :]

    def row_copy(c, who, to):
        return pltpu.make_async_remote_copy(
            src_ref=block(c, who), dst_ref=block(c, who),
            send_sem=row_send.at[c], recv_sem=row_recv.at[c, who], device_id={"row": to},
        )

    def arrived(c, who):
        row_copy(c, who, y_up).wait_recv()

    barrier = pltpu.get_barrier_semaphore()

    def greet(j, carry):
        pl.semaphore_signal(barrier, inc=1, device_id={"section": lax.rem(s + j, n_sec)})
        return carry
    lax.fori_loop(1, n_sec, greet, 0)
    for to in (y_up, y_down):
        pl.semaphore_signal(barrier, inc=1, device_id={"row": to})
    for w in (here + 1, here - 1):
        pl.semaphore_signal(barrier, inc=1, device_id=ring_device(w))

    for e in range(n_sec):
        ids = lax.broadcasted_iota(jnp.int32, (toks.shape[1], cap), 0)
        chosen[:, e * cap : (e + 1) * cap] = (ids == slot_ref[0, e : e + 1, :]).astype(jnp.bfloat16)

    pl.semaphore_wait(barrier, n_sec + 3)

    def tok_at(w):
        w = lax.rem(w + n_ring, n_ring)
        return toks.at[lax.rem(w, 2), pl.ds(pl.multiple_of(w // 2 * n_tok, n_tok), n_tok), :]

    def tok_copy(w, way, src=None):
        return pltpu.make_async_remote_copy(
            src_ref=tok_at(w) if src is None else src, dst_ref=tok_at(w),
            send_sem=tok_send.at[way], recv_sem=tok_recv.at[lax.rem(w + n_ring, n_ring)],
            device_id=ring_device(here + 1 - 2 * way),
        )

    def tok_wait(w):
        tok_copy(w, 0).wait_recv()

    def tok_pass(h):
        origin = lax.rem(here + h, 2)

        @pl.when(h <= n_col - origin)
        def _():
            tok_wait(here - h)

        @pl.when(h < n_col - origin)
        def _():
            tok_copy(here - h, 0).start()

        @pl.when(h <= n_col - 1 + origin)
        def _():
            tok_wait(here + h)

        @pl.when(h < n_col - 1 + origin)
        def _():
            tok_copy(here + h, 1).start()

    tok_copy(here, 0, tok_ref).start()
    tok_copy(here, 1, tok_ref).start()
    tok_own = pltpu.make_async_copy(tok_ref, tok_at(here), tok_recv.at[here])
    tok_own.start()

    def sec_issue(c):
        def from_ref(ref, first_chunk):
            cols = pl.ds(pl.multiple_of((c - first_chunk) * wide, wide), wide)

            def one(j, carry):
                to = lax.rem(s + j, n_sec)
                pltpu.make_async_remote_copy(
                    src_ref=ref.at[0, to, :, cols], dst_ref=piece(c, s),
                    send_sem=sec_send.at[c], recv_sem=sec_recv.at[c], device_id={"section": to},
                ).start()
                return carry
            lax.fori_loop(1, n_sec, one, 0)
            pltpu.make_async_copy(ref.at[0, s, :, cols], piece(c, s), sec_recv.at[c]).start()

        @pl.when(c < half)
        def _():
            from_ref(gate_ref, 0)

        @pl.when(c >= half)
        def _():
            from_ref(up_ref, half)

    def sec_wait(c):
        pltpu.make_async_remote_copy(
            src_ref=block(c, r), dst_ref=block(c, r), send_sem=sec_send.at[c],
            recv_sem=sec_recv.at[c], device_id={"section": lax.rem(s + 1, n_sec)},
        ).wait_recv()

    def open_src(i):
        return up_ref.at[0, :, :, pl.ds((half - OPEN + i) * wide, wide)]

    def open_local(i):
        return pltpu.make_async_copy(open_src(i), block(NC + i, r), row_recv.at[NC + i, r])

    def open_own(i, to):
        pltpu.make_async_remote_copy(
            src_ref=open_src(i), dst_ref=block(NC + i, r),
            send_sem=row_send.at[NC + i], recv_sem=row_recv.at[NC + i, r], device_id={"row": to},
        ).start()

    for i in range(OPEN):
        open_local(i).start()
        open_own(i, y_up)
        open_own(i, y_down)
    open_own(0, z_other)

    for c in range(LEAD):
        sec_issue(c)

    def features(which):
        return lax.rem(z + 1 + which, 2)

    def lhs_at(which, group):
        return lhs.at[which, :, pl.ds(pl.multiple_of(group * cap, cap), cap)]

    def pick(which):
        found = jnp.dot(
            toks[features(which)].T, chosen[...], preferred_element_type=jnp.float32
        ).astype(jnp.bfloat16)
        for e in range(n_sec):
            picked[which, e] = found[:, e * cap : (e + 1) * cap]

    def pick_issue(which):
        def one(j, carry):
            to = lax.rem(s + j, n_sec)
            pltpu.make_async_remote_copy(
                src_ref=picked.at[which, to], dst_ref=lhs_at(which, s), send_sem=pick_send.at[which],
                recv_sem=pick_recv.at[which], device_id={"section": to},
            ).start()
            return carry
        lax.fori_loop(1, n_sec, one, 0)
        lhs[which, :, pl.ds(pl.multiple_of(s * cap, cap), cap)] = picked[which, s]

    def pick_wait(which):
        most = lhs.at[which, :, pl.ds(0, (n_sec - 1) * cap)]
        pltpu.make_async_remote_copy(
            src_ref=most, dst_ref=most, send_sem=pick_send.at[which], recv_sem=pick_recv.at[which],
            device_id={"section": lax.rem(s + 1, n_sec)},
        ).wait_recv()

    def active(c):
        return jnp.logical_not(paired(c)) | (plane(c) == z)

    def own_z(c):
        @pl.when(jnp.logical_not(paired(c)) | (plane(c) != z))
        def _():
            row_copy(c, r, z_other).start()

    def own_y(c):
        @pl.when(active(c))
        def _():
            row_copy(c, r, y_up).start()
            row_copy(c, r, y_down).start()

    def other_y(c):
        arrived(c, z_other)
        row_copy(c, z_other, y_up).start()
        row_copy(c, z_other, y_down).start()

    def pass_up(c):
        arrived(c, y_down)
        row_copy(c, y_down, y_up).start()

    def pass_down(c):
        arrived(c, up_other)
        row_copy(c, up_other, y_down).start()

    def if_active(c, do):
        @pl.when(active(c))
        def _():
            do(c)

    def pass_both(c):
        pass_up(c)
        pass_down(c)

    def rest(c):
        for who in (y_up, far, down_other, far_other):
            arrived(c, who)

    def open_exchange(i):
        open_local(i).wait()
        rest(NC + i)

        def one(j, carry):
            to = lax.rem(s + j, n_sec)
            pltpu.make_async_remote_copy(
                src_ref=grads.at[NC + i, to], dst_ref=grads.at[LOOP + i, s],
                send_sem=sec_send.at[LOOP + i], recv_sem=sec_recv.at[LOOP + i], device_id={"section": to},
            ).start()
            return carry
        lax.fori_loop(1, n_sec, one, 0)
        grads[LOOP + i, s] = grads[NC + i, s]

    def open_most(i):
        most = grads.at[LOOP + i, pl.ds(0, n_sec - 1)]
        return pltpu.make_async_remote_copy(
            src_ref=most, dst_ref=most, send_sem=sec_send.at[LOOP + i], recv_sem=sec_recv.at[LOOP + i],
            device_id={"section": lax.rem(s + 1, n_sec)},
        )

    def open_finish(i):
        open_most(i).wait_recv()
        product_own(LOOP + i)

    def product(which, c):
        return jnp.dot(
            lhs[which], grads[c].reshape(lhs.shape[2], wide), preferred_element_type=jnp.float32
        ).astype(jnp.bfloat16)

    def columns(c, do):
        @pl.when(c < half)
        def _():
            do(out_gate, pl.ds(pl.multiple_of(c * wide, wide), wide))

        @pl.when(c >= half)
        def _():
            do(out_up, pl.ds(pl.multiple_of((c - half) * wide, wide), wide))

    def product_own(c):
        summed = product(1, c)

        def put(ref, cols):
            ref[0, :, cols] = summed
        columns(c, put)

    def out_issue(q):
        def send(ref, cols):
            pltpu.make_async_remote_copy(
                src_ref=stage.at[q], dst_ref=ref.at[0, :, cols],
                send_sem=out_send.at[q], recv_sem=out_recv.at[q], device_id={"row": z_other},
            ).start()
        columns(pair_start(q) + lax.rem(z + q, 2), send)

    def out_copy(q):
        return pltpu.make_async_remote_copy(
            src_ref=stage.at[q], dst_ref=stage.at[q], send_sem=out_send.at[q], recv_sem=out_recv.at[q],
            device_id={"row": z_other},
        )

    def other_step(q):
        return jnp.maximum(pair_start(q) + LAG2 + 1, OTHER0)

    def own_step(q):
        return jnp.maximum(pair_start(q) + LAG2 + 3, OWN0 + q)

    def step(t, carry):
        @pl.when(t + AHEAD < LOOP)
        def _():
            sec_wait(t + AHEAD)
            own_z(t + AHEAD)

        def out_step(q, carry):
            @pl.when(t == other_step(q) + 1)
            def _():
                out_issue(q)
            return carry
        lax.fori_loop(0, PAIRS, out_step, 0)

        @pl.when(t < LOOP)
        def _():
            own_y(t)

        @pl.when(t == BEGIN)
        def _():
            pick_issue(1)

        @pl.when(t < LOOP + LAGZ)
        def _():
            if_active(t - LAGZ, other_y)

        @pl.when(t < LOOP + LAG1)
        def _():
            if_active(t - LAG1, pass_both)

        for i in range(OPEN):
            @pl.when(t == BEGIN + 1 + i)
            def _():
                open_exchange(i)

        @pl.when((t >= LOOP) & (t < NC))
        def _():
            open_finish(t - LOOP)

        def pair(q, carry):
            @pl.when(t == other_step(q))
            def _():
                @pl.when(q == 0)
                def _():
                    pick_wait(0)
                rest(pair_start(q) + lax.rem(z + q, 2))
                stage[q] = product(0, pair_start(q) + lax.rem(z + q, 2))

            @pl.when(t == own_step(q))
            def _():
                product_own(pair_start(q) + lax.rem(z + q, 2))
            return carry

        @pl.when(t == OWN0)
        def _():
            pick_wait(1)
        lax.fori_loop(0, PAIRS, pair, 0)

        plain = t - LAG3

        @pl.when((t >= OWN0) & jnp.logical_not(paired(plain)))
        def _():
            rest(plain)
            product_own(plain)
        return carry

    tok_pass(1)
    for i in range(1, OPEN):
        open_own(i, z_other)
    sec_wait(0)
    own_z(0)
    own_y(0)
    pass_up(NC)
    sec_wait(1)
    own_z(1)
    own_y(1)
    other_y(NC)
    sec_issue(LEAD)
    sec_issue(LEAD + 1)
    sec_wait(2)
    own_y(2)
    for i in range(1, OPEN):
        pass_up(NC + i)
    tok_pass(2)
    for c in (3, 4):
        sec_wait(c)
        own_y(c)
    for c in range(LEAD + 2, BEHIND):
        sec_issue(c)
    for i in range(1, OPEN):
        other_y(NC + i)
    if_active(0, other_y)
    if_active(1, other_y)
    pass_down(NC)
    if n_ring // 2 > 2:
        tok_pass(3)
    pick(0)
    for c in (2, 3, 4):
        own_z(c)
    pick_issue(0)
    for c in range(BEHIND, LOOP):
        sec_issue(c)
    for c in range(5, BEGIN + AHEAD):
        sec_wait(c)
        own_z(c)
        if c < BEGIN:
            own_y(c)
    for i in range(1, OPEN):
        pass_down(NC + i)
    if_active(0, pass_both)
    if_active(1, pass_both)
    if n_ring // 2 > 3:
        tok_pass(4)
    tok_own.wait()
    pick(1)
    if_active(2, other_y)
    if_active(3, other_y)
    if_active(4, other_y)
    lax.fori_loop(BEGIN, LOOP + LAG3, step, 0)

    def sent(ref, sem):
        pltpu.make_async_remote_copy(
            src_ref=ref, dst_ref=ref, send_sem=sem, recv_sem=row_recv.at[0, 0], device_id={"row": y_up},
        ).wait_send()

    def drain_out(q, carry):
        out_copy(q).wait_recv()
        out_copy(q).wait_send()
        return carry
    lax.fori_loop(0, PAIRS, drain_out, 0)

    sent(toks.at[0, pl.ds(0, (n_col - 1) * n_tok), :], tok_send.at[z])
    sent(toks.at[0], tok_send.at[1 - z])
    for which in range(2):
        sent(lhs.at[which, :, pl.ds(0, (n_sec - 1) * cap)], pick_send.at[which])

    def drain(c, carry):
        sent(grads.at[c, pl.ds(0, n_sec - 1), pl.ds(0, rows), :], sec_send.at[c])

        @pl.when(jnp.logical_not(paired(c)))
        def _():
            sent(grads.at[c, :, pl.ds(0, 7 * rows), :], row_send.at[c])

        @pl.when(paired(c) & active(c))
        def _():
            sent(grads.at[c, :, pl.ds(0, 6 * rows), :], row_send.at[c])

        @pl.when(jnp.logical_not(active(c)))
        def _():
            sent(grads.at[c, :, pl.ds(0, rows), :], row_send.at[c])
        return carry
    lax.fori_loop(0, LOOP, drain, 0)
    for i in range(OPEN):
        open_most(i).wait_send()
        sent(grads.at[NC, :, pl.ds(0, 7 * rows), :], row_send.at[NC + i])


def body(n_sec, n_col, tokens, grad_gate, grad_up, slot_token):
    n_tok, d = tokens.shape
    _, e, rows, f = grad_gate.shape
    cap = slot_token.shape[2]
    wide = 2 * f // NC
    n_row = cap // rows
    dma = pltpu.SemaphoreType.DMA
    any_space = pl.BlockSpec(memory_space=pl.ANY)
    vmem = pl.BlockSpec(memory_space=pltpu.VMEM)
    gate, up = pl.pallas_call(
        functools.partial(kernel, n_sec, n_col),
        out_shape=(
            pltpu.VMEM((1, d, f), jnp.bfloat16),
            pltpu.VMEM((1, d, f), jnp.bfloat16),
        ),
        in_specs=[any_space, any_space, any_space, vmem],
        out_specs=(vmem, vmem),
        scratch_shapes=[
            pltpu.VMEM((NC + OPEN, n_sec, cap, wide), jnp.bfloat16),
            pltpu.VMEM((2, n_tok * n_col, d), jnp.bfloat16),
            pltpu.VMEM((n_tok * n_col, n_sec * cap), jnp.bfloat16),
            pltpu.VMEM((2, e, d, cap), jnp.bfloat16),
            pltpu.VMEM((2, d, n_sec * cap), jnp.bfloat16),
            pltpu.VMEM((PAIRS, d, wide), jnp.bfloat16),
            dma((2,)), dma((2 * n_col,)), dma((2,)), dma((2,)),
            dma((NC,)), dma((NC,)), dma((NC + OPEN,)), dma((NC + OPEN, n_row)), dma((PAIRS,)), dma((PAIRS,)),
        ],
        compiler_params=pltpu.CompilerParams(
            collective_id=0, has_side_effects=True, vmem_limit_bytes=50 * 2**20
        ),
        cost_estimate=pl.CostEstimate(
            flops=4 * n_sec * cap * d * f, bytes_accessed=4 * d * f, transcendentals=0
        ),
    )(tokens, grad_gate, grad_up, slot_token)
    shape = jax.ShapeDtypeStruct((1, d, f), jnp.bfloat16)
    return pl.pallas_call(
        settle,
        out_shape=(shape, shape),
        in_specs=[vmem, vmem],
        out_specs=(any_space, any_space),
        scratch_shapes=[dma((2,))],
        compiler_params=pltpu.CompilerParams(vmem_limit_bytes=2 * 2**20),
    )(gate, up)


def settle(gate_in, up_in, gate_out, up_out, sems):
    pieces = 8
    step = gate_in.shape[1] // pieces
    for j, (ref, out) in enumerate(((gate_in, gate_out), (up_in, up_out))):
        for i in range(pieces):
            rows = pl.ds(i * step, step)
            pltpu.make_async_copy(ref.at[:, rows, :], out.at[:, rows, :], sems.at[j]).start()
    pltpu.make_async_copy(gate_in, gate_out, sems.at[0]).wait()
    pltpu.make_async_copy(up_in, up_out, sems.at[1]).wait()


def solution(mesh):
    return jax.shard_map(
        functools.partial(body, mesh.shape["section"], mesh.shape["col"]),
        mesh=mesh,
        in_specs=(
            P(("section", "col"), "row"),
            P("section", None, "row", "col"),
            P("section", None, "row", "col"),
            P("section", None, None),
        ),
        out_specs=(P("section", "row", "col"), P("section", "row", "col")),
        check_vma=False,
    )
```
